32 devices in a mesh: dp: 4 (over y, x), eng: 2 (over core), tp: 4 (over z).
Axes of the slice: x: 2, y: 2, z: 4, core: 2. Of those that a mesh axis runs over, the one named last changes fastest.
Arguments:
- grad_parts: bfloat16 [4, 4, 1024, 14336], P('dp', 'tp', None, 'eng'), may hold values from -24 to 24
- master: float32 [4, 1024, 14336], P('tp', 'dp', 'eng'), may hold values from -0.09375 to 0.09375
- first_moment: float32 [4, 1024, 14336], P('tp', 'dp', 'eng'), may hold values from -12 to 12
- second_moment: float32 [4, 1024, 14336], P('tp', 'dp', 'eng'), may hold values from 4 to 256
- adam_step: int32 [1], replicated, may hold values from 1 to 999
- rank_map: int32 [4], replicated, may hold values from 0 to 3, each once
Outputs:
- new_master: float32 [4, 1024, 14336], P('tp', 'dp', 'eng')
- new_first: float32 [4, 1024, 14336], P('tp', 'dp', 'eng')
- new_second: float32 [4, 1024, 14336], P('tp', 'dp', 'eng')
- rollout: bfloat16 [4, 1024, 2, 4, 1792], P(None, 'dp', None, 'tp')
The draws below stay inside these ranges and needn't reach their ends.
Inputs may be any that keep to these rules, and one draw needn't show every extreme that they name: `rank_map`: each of 0 to 3 appears once.
All inputs are finite; a program needn't handle non-finite values.
Results may differ from the reference program's by a relative error of at most 0.001.
Values may be sent and summed in bfloat16 or wider, within the bound.
A program may use at most 192 MiB of HBM per device.

```python
import math
import jax
import jax.numpy as jnp
from jax import lax

D = 4096
F = 14336
N_DP = 4
N_ENG = 2
N_TP = 4


def with_spikes(drawn, key, source, target, parts, factor):
    def block_of(dim):
        return (jnp.arange(drawn.shape[dim]) // (drawn.shape[dim] // parts)).reshape((-1,) + (1,) * (drawn.ndim - 1 - dim))

    near = jax.random.permutation(key, parts)[block_of(target)]
    second = (block_of(target) + parts // 2) % parts
    return jnp.where((block_of(source) == near) | (block_of(source) == second), factor * drawn, drawn)


def shard_levels(rng, shape, split, low, high):
    loudness, own = 1.0, jax.random.fold_in(rng, 6)
    for dim, parts in split:
        steps = jnp.exp(jax.random.uniform(jax.random.fold_in(own, dim), (parts,), jnp.float32, low / len(split), high / len(split)))
        loudness = loudness * jnp.repeat(steps, shape[dim] // parts).reshape([-1 if axis == dim else 1 for axis in range(len(shape))])
    return loudness


def centred(rng, dims, width, limit, split=(), dtype=jnp.bfloat16):
    level = shard_levels(rng, dims, split, -0.22, 0.18) if split else 1.0
    drawn = jax.random.normal(rng, dims, jnp.float32) * width * level
    return jnp.minimum(jnp.maximum(drawn, -limit), limit).astype(dtype)


def heavy_noise(stream_key, dims, width, most, shards, heavy, kind=jnp.bfloat16):
    drawn = width * jax.random.normal(stream_key, dims, jnp.float32)
    if shards:
        drawn = drawn * shard_levels(stream_key, dims, shards, -0.22, 0.18)
    return jnp.clip(with_spikes(drawn, jax.random.fold_in(stream_key, 3), *heavy), -most, most).astype(kind)


def setup_inputs(seed: int = 0) -> dict:
    seeds = jax.random.split(jax.random.key(seed), 7)
    return {
        "grad_parts": heavy_noise(seeds[0], (N_DP, N_TP, D // N_TP, F), 4.0, 24.0, ((0, 4), (1, 4), (3, 2)), (0, 2, 4, 2.0)),
        "master": centred(seeds[1], (N_TP, D // N_TP, F), D ** -0.5, 0.09375, ((0, 4), (1, 4), (2, 2)), jnp.float32),
        "first_moment": centred(seeds[2], (N_TP, D // N_TP, F), 2.0, 12.0, ((0, 4), (1, 4), (2, 2)), jnp.float32),
        "second_moment": jnp.clip(jnp.exp(math.log(256.0) - 4.158883 * jax.random.uniform(seeds[3], (N_TP, D // N_TP, F), jnp.float32) ** shard_levels(seeds[3], (N_TP, D // N_TP, F), ((0, 4), (1, 4), (2, 2)), -0.2, 0.2)), 4.0, 256.0),
        "adam_step": jax.random.randint(seeds[4], (1,), 1, 1000).astype(jnp.int32),
        "rank_map": jax.random.permutation(seeds[5], N_TP).astype(jnp.int32),
    }


beta_one = 0.9
beta_two = 0.95
rate_value = 0.001
decay_value = 0.01
eps_value = 1e-08

def reference(grad_parts, master, first_moment, second_moment, adam_step, rank_map):
    summed = lax.optimization_barrier(jnp.sum(grad_parts.astype(jnp.float32), axis=0))
    count = adam_step[0].astype(jnp.float32)
    new_first = beta_one * first_moment + (1.0 - beta_one) * summed
    new_second = beta_two * second_moment + (1.0 - beta_two) * summed * summed
    first_hat = new_first / (1.0 - jnp.power(beta_one, count))
    second_hat = new_second / (1.0 - jnp.power(beta_two, count))
    new_master = master - rate_value * (first_hat / (jnp.sqrt(second_hat) + eps_value) + decay_value * master)
    weights = new_master.astype(jnp.bfloat16).reshape(N_TP, D // N_TP, N_ENG, N_TP, F // (N_ENG * N_TP))
    rollout = jnp.take(weights, rank_map.astype(jnp.int32), axis=3)
    return (new_master, new_first, new_second, rollout)
```

```python
import functools
import jax
import jax.numpy as jnp
from jax import lax
from jax.experimental import pallas as pl
from jax.experimental.pallas import tpu as pltpu
from jax.sharding import PartitionSpec as P

beta_one = 0.9
beta_two = 0.95
rate_value = 0.001
decay_value = 0.01
eps_value = 1e-08

CHUNKS = 4
TILE = 16


def corrections(adam_step):
    count = adam_step[0].astype(jnp.float32)
    return 1.0 - jnp.power(beta_one, count), 1.0 - jnp.power(beta_two, count)


def plain_shards(grad_parts, master, first_moment, second_moment, adam_step, rank_map):
    summed = lax.psum_scatter(grad_parts.astype(jnp.float32), "dp", scatter_dimension=2, tiled=True)
    summed = summed.reshape(master.shape)
    fix_one, fix_two = corrections(adam_step)
    new_first = beta_one * first_moment + (1.0 - beta_one) * summed
    new_second = beta_two * second_moment + (1.0 - beta_two) * summed * summed
    first_hat = new_first / fix_one
    second_hat = new_second / fix_two
    new_master = master - rate_value * (
        first_hat / (jnp.sqrt(second_hat) + eps_value) + decay_value * master
    )
    row_count = master.shape[1]
    ranks = lax.axis_size("tp")
    block_width = master.shape[2] // ranks
    piece = new_master.astype(jnp.bfloat16).reshape(1, row_count, 1, ranks, block_width)
    ordered = jnp.take(piece, rank_map, axis=3)
    placed = lax.all_to_all(ordered, "tp", split_axis=3, concat_axis=0, tiled=True)
    rollout = lax.all_gather(placed, "eng", axis=2, tiled=True)
    return (new_master, new_first, new_second, rollout)


def adam_kernel(parts, ranks, aliased, place, order, scales, *refs):
    grads, refs = refs[:parts], refs[parts:]
    master, first, second = refs[:3]
    refs = refs[3 + (3 if aliased else 0):]
    new_master, new_first, new_second = refs[:3]
    sends, held = refs[3:-1], refs[-1]
    width = held.shape[2]
    scale_one, scale_two = scales[0], scales[1]
    for block in range(ranks):
        columns = pl.ds(block * width, width)
        summed = grads[0][:, columns].astype(jnp.float32)
        for part in grads[1:]:
            summed += part[:, columns].astype(jnp.float32)
        first_now = beta_one * first[:, columns] + (1.0 - beta_one) * summed
        second_now = beta_two * second[:, columns] + (1.0 - beta_two) * summed * summed
        old = master[:, columns]
        step = (first_now * scale_one) / (jnp.sqrt(second_now * scale_two) + eps_value)
        now = old - rate_value * (step + decay_value * old)
        new_first[:, columns] = first_now
        new_second[:, columns] = second_now
        new_master[:, columns] = now
        held[block] = now.astype(jnp.bfloat16)
    for hop in range(ranks):
        sends[hop][...] = held[order[hop]]


def adam_chunk(chunk, rows, place, order, scales, grad, received, states, outs):
    columns = grad.shape[1]
    ranks = order.shape[0]
    width = columns // ranks
    tiles = rows // TILE
    all_tiles = states[0].shape[0] // TILE
    base = chunk * tiles
    own = pl.BlockSpec((TILE, columns), lambda i, p, o, s: (p[0] * all_tiles + base + i, 0))
    local = pl.BlockSpec((TILE, columns), lambda i, p, o, s: (i, 0))
    whole = pl.BlockSpec((TILE, columns), lambda i, p, o, s: (base + i, 0))
    send = pl.BlockSpec((TILE, width), lambda i, p, o, s: (i, 0))
    parts = 1 + len(received)
    aliased = outs is not None
    first_out = 3 + parts + 3
    return pl.pallas_call(
        functools.partial(adam_kernel, parts, ranks, aliased),
        out_shape=[jax.ShapeDtypeStruct(s.shape, s.dtype) for s in states]
        + [jax.ShapeDtypeStruct((rows, width), jnp.bfloat16)] * ranks,
        grid_spec=pltpu.PrefetchScalarGridSpec(
            num_scalar_prefetch=3,
            grid=(tiles,),
            in_specs=[own] + [local] * len(received) + [whole] * 3
            + ([pl.BlockSpec(memory_space=pl.ANY)] * 3 if aliased else []),
            out_specs=[whole] * 3 + [send] * ranks,
            scratch_shapes=[pltpu.VMEM((ranks, TILE, width), jnp.bfloat16)],
        ),
        input_output_aliases={first_out + i: i for i in range(3)} if aliased else {},
        cost_estimate=pl.CostEstimate(
            flops=20 * rows * columns, bytes_accessed=34 * rows * columns, transcendentals=rows * columns
        ),
        name=f"adam{chunk}",
    )(place, order, scales, grad, *received, *states, *(outs if aliased else ()))


def shards(grad_parts, master, first_moment, second_moment, adam_step, rank_map):
    replicas, ranks = lax.axis_size("dp"), lax.axis_size("tp")
    row_count, columns = master.shape[1], master.shape[2]
    width = columns // ranks
    rows = row_count // CHUNKS
    me_dp, me_tp, me_eng = (lax.axis_index(a) for a in ("dp", "tp", "eng"))
    grad = grad_parts.reshape(grad_parts.shape[2], columns)
    states = [s.reshape(row_count, columns) for s in (master, first_moment, second_moment)]
    place = me_dp.reshape(1).astype(jnp.int32)
    order = lax.dynamic_slice(jnp.concatenate([rank_map, rank_map]), (me_tp,), (ranks,))
    scales = jnp.stack([1.0 / value for value in corrections(adam_step)])

    received = []
    for chunk in range(CHUNKS):
        got = []
        for hop in range(1, replicas):
            start = (me_dp ^ hop) * row_count + chunk * rows
            piece = lax.dynamic_slice(grad, (start, 0), (rows, columns))
            got.append(lax.ppermute(piece, "dp", [(i, i ^ hop) for i in range(replicas)]))
        received.append(got)

    outs = None
    rollout = jnp.zeros((ranks, row_count, 2, 1, width), jnp.bfloat16)
    for chunk in range(CHUNKS):
        results = adam_chunk(chunk, rows, place, order, scales, grad, received[chunk], states, outs)
        outs, sends = results[:3], results[3:]
        for hop in range(ranks):
            mine = sends[hop]
            if hop:
                mine = lax.ppermute(mine, "tp", [(i, (i + hop) % ranks) for i in range(ranks)])
            other = lax.ppermute(mine, "eng", [(0, 1), (1, 0)])
            low = jnp.where(me_eng == 0, mine, other)
            high = jnp.where(me_eng == 0, other, mine)
            pair = jnp.stack([low, high], axis=1).reshape(1, rows, 2, 1, width)
            group = (me_tp - hop + ranks) % ranks
            rollout = lax.dynamic_update_slice(rollout, pair, (group, chunk * rows, 0, 0, 0))
    return (*(o.reshape(master.shape) for o in outs), rollout)


def solution(mesh):
    sizes = dict(mesh.shape)

    def step(grad_parts, master, *rest):
        width = master.shape[2] // (sizes["eng"] * sizes["tp"])
        rows = master.shape[1] // sizes["dp"]
        power = sizes["dp"] & (sizes["dp"] - 1) == 0
        fits = width % 128 == 0 and rows % (CHUNKS * TILE) == 0 and sizes["eng"] == 2 and power
        return jax.shard_map(
            shards if fits else plain_shards,
            mesh=mesh,
            in_specs=(
                P("dp", "tp", None, "eng"),
                P("tp", "dp", "eng"),
                P("tp", "dp", "eng"),
                P("tp", "dp", "eng"),
                P(),
                P(),
            ),
            out_specs=(
                P("tp", "dp", "eng"),
                P("tp", "dp", "eng"),
                P("tp", "dp", "eng"),
                P(None, "dp", None, "tp", None),
            ),
            check_vma=False,
        )(grad_parts, master, *rest)

    return step
```
